256 devices in a mesh: tm: 32 (over y, z), space: 8 (over x, core).
Axes of the slice: x: 4, y: 4, z: 8, core: 2. Of those that a mesh axis runs over, the one named last changes fastest.
Arguments:
- forcing: float32 [128, 128, 128, 128], P('tm', 'space'), may hold values from -6 to 6
- coarse_guess: float32 [32, 128, 128, 128], P('tm', 'space'), may hold values from -6 to 6
- initial: float32 [128, 128, 128], P('space'), may hold values from -6 to 6
Outputs:
- solution: float32 [128, 128, 128, 128], P('tm', 'space')
- residual: float32 [32, 128, 128, 128], P('tm', None, 'space')
The draws below stay inside these ranges and needn't reach their ends.
All inputs are finite; a program needn't handle non-finite values.
Results may differ from the reference program's by a relative error of at most 0.00007.
Values sent between devices are 32-bit elements; how exact they have to be, the bound alone decides.
A program may use at most 192 MiB of HBM per device.

```python
import jax
import jax.numpy as jnp
from jax import lax

NX = 128
NY = 128
NZ = 128
COARSEN = 4
STEPS = 128
INTERVALS = 32
N_TM = 32


def levels(key, dims, shards, smallest, top_value):
    def one(position, shards_of):
        draws = jax.random.uniform(jax.random.fold_in(jax.random.fold_in(key, 6), position), (shards_of,), jnp.float32, smallest / len(shards), top_value / len(shards))
        return jnp.repeat(jnp.exp(draws), dims[position] // shards_of).reshape((-1,) + (1,) * (len(dims) - position - 1))

    factor_of = one(*shards[0])
    for cut in shards[1:]:
        factor_of = factor_of * one(*cut)
    return factor_of


def noise(key, extent, deviation, most, pieces=(), held_as=jnp.bfloat16):
    gain = levels(key, extent, pieces, -0.22, 0.18) if pieces else 1.0
    drawn = jax.random.normal(key, extent, jnp.float32) * deviation * gain
    return jnp.minimum(jnp.maximum(drawn, -most), most).astype(held_as)


def setup_inputs(seed: int = 0) -> dict:
    key_list = jax.random.split(jax.random.key(seed), 4)
    forcing = noise(key_list[0], (STEPS, NX, NY, NZ), 1.0, 6.0, ((0, 32), (1, 8)), jnp.float32)
    coarse_guess = noise(key_list[1], (INTERVALS, NX, NY, NZ), 1.0, 6.0, ((0, 32), (1, 8)), jnp.float32)
    initial = noise(key_list[2], (NX, NY, NZ), 1.0, 6.0, ((0, 8),), jnp.float32)
    return dict(forcing=forcing, coarse_guess=coarse_guess, initial=initial)


time_step = 0.5
highest = lax.Precision.HIGHEST

def sine_table(length):
    ladder = jnp.arange(1, length + 1, dtype=jnp.float32)
    return jnp.sqrt(2.0 / (length + 1)) * jnp.sin(jnp.pi * ladder[:, None] * ladder[None, :] / (length + 1))

def eigen_values(length):
    ladder = jnp.arange(1, length + 1, dtype=jnp.float32)
    return -4.0 * jnp.sin(jnp.pi * ladder / (2 * (length + 1))) ** 2

def all_modes(fields, table_x, table_y, table_z):
    fields = jnp.einsum('bxyz,zr->bxyr', fields, table_z, precision=highest)
    fields = jnp.einsum('bxyr,yq->bxqr', fields, table_y, precision=highest)
    return jnp.einsum('bxqr,xp->bpqr', fields, table_x, precision=highest)

def reference(forcing, coarse_guess, initial):
    table_x = sine_table(NX)
    table_y = sine_table(NY)
    table_z = sine_table(NZ)
    spectrum = eigen_values(NX)[:, None, None] + eigen_values(NY)[None, :, None] + eigen_values(NZ)[None, None, :]
    implicit = 1.0 - 0.5 * time_step * spectrum
    fine_rate = (1.0 + 0.5 * time_step * spectrum) / implicit
    wide_step = 0.5 * COARSEN * time_step
    coarse_rate = (1.0 + wide_step * spectrum) / (1.0 - wide_step * spectrum)
    blocks = forcing.reshape(N_TM, COARSEN, NX, NY, NZ)
    source = lax.map(lambda block: all_modes(block, table_x, table_y, table_z) * (time_step / implicit), blocks)
    anchor = all_modes(initial[None], table_x, table_y, table_z)
    firsts = jnp.concatenate([coarse_guess[-1:], coarse_guess[:-1]], axis=0)
    begin = lax.map(lambda field: all_modes(field[None], table_x, table_y, table_z)[0], firsts)

    def relax_steps(starting):
        current = starting
        values = []
        for number in range(COARSEN - 1):
            current = fine_rate * current + source[:, number]
            values.append(current)
        return values
    coarse_value = fine_rate * relax_steps(begin)[-1] + source[:, COARSEN - 1]
    second = jnp.concatenate([anchor, coarse_value[:-1]], axis=0)
    residual = fine_rate * relax_steps(second)[-1] + source[:, COARSEN - 1] - coarse_value

    def sweep(error, term):
        error = coarse_rate * error + term
        return (error, error)
    _, errors = lax.scan(sweep, jnp.zeros_like(anchor[0]), residual)
    corrected = coarse_value + errors
    third = jnp.concatenate([anchor, corrected[:-1]], axis=0)
    points = relax_steps(third) + [corrected]
    stacked = jnp.stack(points, axis=1)
    cells = lax.map(lambda block: all_modes(block, table_x, table_y, table_z), stacked)
    return (cells.reshape(COARSEN * N_TM, NX, NY, NZ), residual)
```

```python
import jax
import jax.numpy as jnp
import numpy as np
from jax import lax
from jax.experimental import pallas as pl
from jax.experimental.pallas import tpu as pltpu
from jax.sharding import PartitionSpec as P

MESH = pl.DeviceIdType.MESH
F32, BF16 = jnp.float32, jnp.bfloat16
N = 128
SPACE = 8
TM = 32
STEPS = 4
TIME_STEP = 0.5
HALVES = 2
PAIRS = 4


def split_parts(table):
    high = table.astype(BF16)
    return high, (table - high.astype(np.float64)).astype(BF16)


def sine_table(length):
    ladder = np.arange(1, length + 1, dtype=np.float64)
    return np.sqrt(2.0 / (length + 1)) * np.sin(np.pi * ladder[:, None] * ladder[None, :] / (length + 1))


def eigen_values(length):
    ladder = np.arange(1, length + 1, dtype=np.float64)
    return -4.0 * np.sin(np.pi * ladder / (2 * (length + 1))) ** 2


def left_table(rows):
    high, low = split_parts(rows)
    return np.concatenate(
        [np.concatenate([high, high], axis=-1), np.concatenate([low, low], axis=-1)], axis=-2
    )


def tables():
    sine = sine_table(N)
    left = left_table(sine)
    right = np.ascontiguousarray(left.T)
    chosen = sine.reshape(SPACE, HALVES, PAIRS, 2, N).transpose(2, 0, 1, 3, 4).reshape(PAIRS, 32, N)
    anchor_y = left_table(chosen)
    anchor_x = left_table(sine.reshape(8, 16, N))
    line = eigen_values(N)
    plane = np.tile(line[:, None] + line[None, :], (1, 2)).astype(np.float32)
    along_y = np.repeat(line.reshape(SPACE, 8, 2), N, axis=2).astype(np.float32)
    return right, left, anchor_y, anchor_x, plane, along_y


def two_parts(value, axis):
    high = value.astype(BF16)
    low = (value - high.astype(F32)).astype(BF16)
    return jnp.concatenate([high, low], axis=axis)


def along_rows(value, right_ref):
    made = jnp.dot(two_parts(value, 1), right_ref[...], preferred_element_type=F32)
    return made[:, :N] + made[:, N:]


def along_columns(left, value):
    made = jnp.dot(left, two_parts(value, 0), preferred_element_type=F32)
    half = made.shape[0] // 2
    return made[:half] + made[half:]


def kernel(
    forcing_ref, guess_ref, initial_ref, right_ref, left_ref, anchor_y_ref, anchor_x_ref, plane_ref, along_y_ref,
    solution_ref, residual_ref,
    cells, first_cells, sent, received, anchor_rows, anchor_sent, anchor_received, anchor,
    fine, weight, coarse, guess, begin, parts, change, change_before, scan_in, scan_out, error_before,
    back_sent, back_received, made, residual,
    load_sem, store_sem, x_send, x_recv, anchor_send, anchor_recv, shift_send, shift_recv,
    scan_send, scan_recv, error_send, error_recv, back_send, back_recv,
):
    t, s = lax.axis_index("tm"), lax.axis_index("space")
    after = lax.rem(t + 1, TM)

    loads = [pltpu.make_async_copy(guess_ref.at[0], cells.at[0], load_sem.at[0])]
    loads += [pltpu.make_async_copy(forcing_ref.at[k], cells.at[k + 1], load_sem.at[k + 1]) for k in range(STEPS)]
    loads += [pltpu.make_async_copy(initial_ref, first_cells, load_sem.at[5])]
    for load in loads:
        load.start()

    barrier = pltpu.get_barrier_semaphore()
    for k in range(1, SPACE):
        pl.semaphore_signal(barrier, inc=1, device_id=(t, lax.rem(s + k, SPACE)), device_id_type=MESH)

    @pl.loop(1, TM)
    def _(k):
        pl.semaphore_signal(barrier, inc=1, device_id=(lax.rem(t + k, TM), s), device_id_type=MESH)

    def remote(src, dst, send, recv, tm, space):
        return pltpu.make_async_remote_copy(
            src_ref=src, dst_ref=dst, send_sem=send, recv_sem=recv, device_id=(tm, space), device_id_type=MESH
        )

    def arrived(like, send, recv):
        remote(like, like, send, recv, after, s).wait_recv()

    def left_here(like, send, recv):
        remote(like, like, send, recv, after, s).wait_send()

    def to_modes(field):
        @pl.loop(0, 4)
        def _(i):
            block = cells[field, pl.ds(4 * i, 4)].reshape(4 * N, N)
            block = along_rows(block, right_ref)
            for pair in range(2):
                both = jnp.concatenate([block[(2 * pair + u) * N : (2 * pair + u + 1) * N] for u in range(2)], axis=1)
                both = along_columns(left_ref[...], both)
                for u in range(2):
                    one = both[:, u * N : (u + 1) * N].reshape(SPACE, HALVES, 8, N)
                    x = 4 * i + 2 * pair + u
                    for h in range(HALVES):
                        sent[2 * field + h, :, pl.ds(pl.multiple_of(8 * x, 8), 8), :] = one[:, h]

    def exchange(field, h):
        at = 2 * field + h
        for k in range(1, SPACE):
            other = lax.rem(s + k, SPACE)
            remote(
                sent.at[at, other], received.at[at, pl.ds(pl.multiple_of(s * N, N), N)],
                x_send.at[at], x_recv.at[at], t, other,
            ).start()
        received[at, pl.ds(pl.multiple_of(s * N, N), N), :] = sent[at, s]

    loads[0].wait()
    to_modes(0)
    pl.semaphore_wait(barrier, SPACE - 1 + TM - 1)
    exchange(0, 0)
    exchange(0, 1)
    for field in range(1, STEPS + 1):
        loads[field].wait()
        to_modes(field)
        exchange(field, 0)
    for field in range(1, STEPS + 1):
        exchange(field, 1)

    loads[5].wait()
    column, block_of = lax.div(t, 8), lax.rem(t, 8)

    @pl.loop(0, 4)
    def _(i):
        for pair in range(2):
            both = jnp.concatenate([first_cells[4 * i + 2 * pair + u] for u in range(2)], axis=1)
            both = along_columns(anchor_y_ref[column], both)
            for u in range(2):
                x = 4 * i + 2 * pair + u
                anchor_rows[pl.ds(pl.multiple_of(32 * x, 32), 32), :] = both[:, u * N : (u + 1) * N]

    anchor_rows[...] = along_rows(anchor_rows[...], right_ref)
    for k in range(32):
        anchor_sent[k // 4, pl.ds(16 * (k % 4), 16), :] = anchor_rows[pl.ds(k, 16, stride=32), :]
    for k in range(1, SPACE):
        other = lax.rem(s + k, SPACE)
        remote(anchor_sent.at[other], anchor_received.at[s], anchor_send, anchor_recv, t, other).start()
    anchor_received[s] = anchor_sent[s]

    @pl.loop(0, HALVES * PAIRS)
    def _(i):
        spectrum = plane_ref[...] + along_y_ref[s, pl.ds(i, 1), :]
        inverse = 1.0 / (1.0 - 0.5 * TIME_STEP * spectrum)
        h, pair = lax.div(i, PAIRS), lax.rem(i, PAIRS)
        fine[h, pair] = (1.0 + 0.5 * TIME_STEP * spectrum) * inverse
        weight[h, pair] = TIME_STEP * inverse
        wide = 0.5 * STEPS * TIME_STEP
        coarse[h, pair] = (1.0 + wide * spectrum) / (1.0 - wide * spectrum)

    def lines(at, pair):
        return jnp.concatenate(
            [received[at, pl.ds(2 * pair + u, N, stride=8), :] for u in range(2)], axis=1
        )

    for h in range(HALVES):
        arrived(received.at[h, pl.ds(0, 7 * N)], x_send.at[h], x_recv.at[h])

        @pl.loop(0, PAIRS)
        def _(pair):
            guess[h, pair] = along_columns(left_ref[...], lines(h, pair))

        remote(guess.at[h], begin.at[h], shift_send.at[h], shift_recv.at[h], after, s).start()

    def relax(h):
        for field in range(1, STEPS + 1):
            at = 2 * field + h
            arrived(received.at[at, pl.ds(0, 7 * N)], x_send.at[at], x_recv.at[at])

            @pl.loop(0, PAIRS)
            def _(pair):
                source = along_columns(left_ref[...], lines(at, pair)) * weight[h, pair]
                if field > 1:
                    source = source + fine[h, pair] * parts[field - 2, h, pair]
                parts[field - 1, h, pair] = source

        arrived(begin.at[h], shift_send.at[h], shift_recv.at[h])

        @pl.loop(0, PAIRS)
        def _(pair):
            square = fine[h, pair] * fine[h, pair]
            value = square * square * begin[h, pair] + parts[3, h, pair]
            parts[3, h, pair] = value
            known = guess[h, pair]
            change[h, pair] = jnp.where(t == TM - 1, known, value - known)

        @pl.loop(1, TM)
        def _(k):
            other = lax.rem(t + k, TM)
            rows = pl.ds(pl.multiple_of(16 * lax.rem(other, 8), 16), 16)
            remote(
                change.at[h, lax.div(other, 8), rows], scan_in.at[h, t], scan_send.at[h], scan_recv.at[h], other, s
            ).start()

        mine = pl.ds(pl.multiple_of(16 * block_of, 16), 16)
        scan_in[h, t] = change[h, column, mine, :]
        remote(change.at[h], change_before.at[h], shift_send.at[2 + h], shift_recv.at[2 + h], after, s).start()

    def scan(h):
        arrived(scan_in.at[h, pl.ds(0, TM - 1)], scan_send.at[h], scan_recv.at[h])
        mine = pl.ds(pl.multiple_of(16 * block_of, 16), 16)
        square = fine[h, column, mine, :] * fine[h, column, mine, :]
        power, rate = square * square, coarse[h, column, mine, :]
        first = anchor[h] - scan_in[h, TM - 1]
        scan_out[h, 0] = first

        def sweep(j, error):
            scan_out[h, j] = error
            return rate * error + power * scan_in[h, j - 1]

        scan_out[h, TM - 1] = lax.fori_loop(1, TM - 1, sweep, power * first)

        @pl.loop(1, TM)
        def _(k):
            other = lax.rem(t + k, TM)
            remote(
                scan_out.at[h, other], error_before.at[h, column, mine], error_send.at[h], error_recv.at[h], other, s
            ).start()

        error_before[h, column, mine, :] = scan_out[h, t]

    def go_back(h):
        arrived(change_before.at[h], shift_send.at[2 + h], shift_recv.at[2 + h])
        arrived(scan_out.at[h, pl.ds(0, TM - 1)], error_send.at[h], error_recv.at[h])

        @pl.loop(0, PAIRS)
        def _(pair):
            came = error_before[h, pair]
            delta = jnp.where(t == 0, came, change_before[h, pair])
            error = jnp.where(t == 0, jnp.zeros_like(came), came)
            rate = fine[h, pair]
            square = rate * rate
            gap = square * square * delta
            for u in range(2):
                residual[pl.ds(8 * h + 2 * pair + u, N, stride=16), :] = gap[:, u * N : (u + 1) * N]
            third = begin[h, pair] + (delta + error)
            for k in range(STEPS):
                if k == 0:
                    point = rate * third + parts[0, h, pair]
                elif k == 1:
                    point = square * third + parts[1, h, pair]
                elif k == 2:
                    point = rate * square * third + parts[2, h, pair]
                else:
                    point = parts[3, h, pair] + (gap + coarse[h, pair] * error)
                point = along_columns(left_ref[...], point)
                for u in range(2):
                    rows = pl.ds(pl.multiple_of(32 * pair + 16 * u, 16), 16)
                    back_sent[2 * k + h, :, rows, :] = point[:, u * N : (u + 1) * N].reshape(SPACE, 16, N)

        for k in range(STEPS):
            at = 2 * k + h
            slot = pl.ds(pl.multiple_of(256 * s + 128 * h, 128), 128)
            for hop in range(1, SPACE):
                other = lax.rem(s + hop, SPACE)
                remote(
                    back_sent.at[at, other], back_received.at[k, slot], back_send.at[at], back_recv.at[at], t, other
                ).start()
            back_received[k, slot, :] = back_sent[at, s]

    relax(0)
    arrived(anchor_received.at[pl.ds(0, SPACE - 1)], anchor_send, anchor_recv)
    for h in range(HALVES):
        both = jnp.concatenate(
            [anchor_received[:, pl.ds(32 * h + 16 * u, 16), :].reshape(N, N) for u in range(2)], axis=1
        )
        anchor[h] = along_columns(anchor_x_ref[block_of], both)
    scan(0)
    relax(1)
    go_back(0)
    scan(1)
    go_back(1)
    pltpu.make_async_copy(residual, residual_ref, store_sem.at[STEPS]).start()

    stores = []
    for k in range(STEPS):
        for h in range(HALVES):
            at = 2 * k + h
            arrived(back_received.at[k, pl.ds(0, 7 * N)], back_send.at[at], back_recv.at[at])

        @pl.loop(0, 4)
        def _(i):
            pieces = []
            for pair in range(2):
                x = 4 * i + 2 * pair
                both = jnp.concatenate(
                    [back_received[k, pl.ds(x + u, N, stride=16), :] for u in range(2)], axis=1
                )
                both = along_columns(left_ref[...], both)
                pieces += [both[:, :N], both[:, N:]]
            block = along_rows(jnp.concatenate(pieces, axis=0), right_ref)
            made[k, pl.ds(4 * i, 4)] = block.reshape(4, N, N)

        stores.append(pltpu.make_async_copy(made.at[k], solution_ref.at[k], store_sem.at[k]))
        stores[-1].start()

    for at in range(2 * (STEPS + 1)):
        left_here(received.at[at, pl.ds(0, 7 * N)], x_send.at[at], x_recv.at[at])
    left_here(anchor_received.at[pl.ds(0, SPACE - 1)], anchor_send, anchor_recv)
    for h in range(HALVES):
        left_here(guess.at[h], shift_send.at[h], shift_recv.at[h])
        left_here(change.at[h], shift_send.at[2 + h], shift_recv.at[2 + h])
        left_here(scan_in.at[h, pl.ds(0, TM - 1)], scan_send.at[h], scan_recv.at[h])
        left_here(scan_out.at[h, pl.ds(0, TM - 1)], error_send.at[h], error_recv.at[h])
    for at in range(2 * STEPS):
        left_here(back_received.at[0, pl.ds(0, 7 * N)], back_send.at[at], back_recv.at[at])
    for store in stores:
        store.wait()
    pltpu.make_async_copy(residual, residual_ref, store_sem.at[STEPS]).wait()


def per_device(forcing, coarse_guess, initial):
    modal = (HALVES, PAIRS, N, 2 * N)
    dma = pltpu.SemaphoreType.DMA
    vmem = pl.BlockSpec(memory_space=pltpu.VMEM)
    anywhere = pl.BlockSpec(memory_space=pl.ANY)
    given = tables()
    out, gap = pl.pallas_call(
        kernel,
        out_shape=(
            jax.ShapeDtypeStruct((STEPS, 16, N, N), F32),
            jax.ShapeDtypeStruct((16 * N, N), F32),
        ),
        in_specs=[anywhere] * 3 + [vmem] * len(given),
        out_specs=(anywhere, anywhere),
        scratch_shapes=[
            pltpu.VMEM((STEPS + 1, 16, N, N), F32),
            pltpu.VMEM((16, N, N), F32),
            pltpu.VMEM((2 * (STEPS + 1), SPACE, N, N), F32),
            pltpu.VMEM((2 * (STEPS + 1), SPACE * N, N), F32),
            pltpu.VMEM((512, N), F32),
            pltpu.VMEM((SPACE, 64, N), F32),
            pltpu.VMEM((SPACE, 64, N), F32),
            pltpu.VMEM((HALVES, 16, 2 * N), F32),
            pltpu.VMEM(modal, F32),
            pltpu.VMEM(modal, F32),
            pltpu.VMEM(modal, F32),
            pltpu.VMEM(modal, F32),
            pltpu.VMEM(modal, F32),
            pltpu.VMEM((STEPS,) + modal, F32),
            pltpu.VMEM(modal, F32),
            pltpu.VMEM(modal, F32),
            pltpu.VMEM((HALVES, TM, 16, 2 * N), F32),
            pltpu.VMEM((HALVES, TM, 16, 2 * N), F32),
            pltpu.VMEM(modal, F32),
            pltpu.VMEM((2 * STEPS, SPACE, N, N), F32),
            pltpu.VMEM((STEPS, 16 * N, N), F32),
            pltpu.VMEM((STEPS, 16, N, N), F32),
            pltpu.VMEM((16 * N, N), F32),
            dma((STEPS + 2,)),
            dma((STEPS + 1,)),
            dma((2 * (STEPS + 1),)),
            dma((2 * (STEPS + 1),)),
            dma,
            dma,
            dma((4,)),
            dma((4,)),
            dma((HALVES,)),
            dma((HALVES,)),
            dma((HALVES,)),
            dma((HALVES,)),
            dma((2 * STEPS,)),
            dma((2 * STEPS,)),
        ],
        compiler_params=pltpu.CompilerParams(
            collective_id=0, has_side_effects=True, vmem_limit_bytes=62 * 1024 * 1024
        ),
    )(forcing, coarse_guess, initial, *given)
    return out, gap.reshape(1, N, 16, N)


def solution(mesh):
    in_specs = (P("tm", "space", None, None), P("tm", "space", None, None), P("space", None, None))
    out_specs = (P("tm", "space", None, None), P("tm", None, "space", None))
    return jax.shard_map(per_device, mesh=mesh, in_specs=in_specs, out_specs=out_specs, check_vma=False)
```

```python
import jax
import jax.numpy as jnp
import numpy as np
from jax import lax
from jax.experimental import pallas as pl
from jax.experimental.pallas import tpu as pltpu
from jax.sharding import PartitionSpec as P

MESH = pl.DeviceIdType.MESH
F32, BF16 = jnp.float32, jnp.bfloat16
N = 128
SPACE = 8
TM = 32
STEPS = 4
TIME_STEP = 0.5
HALVES = 2
PAIRS = 4
CHUNKS = 2
GROUP = PAIRS // CHUNKS
ROWS = N * GROUP // TM
FIELDS = 4
BACK = 3
HALF_STEP = 0.5 * TIME_STEP


def split_parts(table):
    high = table.astype(BF16)
    return high, (table - high.astype(np.float64)).astype(BF16)


def sine_table(length):
    ladder = np.arange(1, length + 1, dtype=np.float64)
    return np.sqrt(2.0 / (length + 1)) * np.sin(np.pi * ladder[:, None] * ladder[None, :] / (length + 1))


def eigen_values(length):
    ladder = np.arange(1, length + 1, dtype=np.float64)
    return -4.0 * np.sin(np.pi * ladder / (2 * (length + 1))) ** 2


def left_table(rows):
    high, low = split_parts(rows)
    return np.concatenate(
        [np.concatenate([high, high], axis=-1), np.concatenate([low, low], axis=-1)], axis=-2
    )


def tables():
    sine = sine_table(N)
    left = left_table(sine)
    right = np.ascontiguousarray(left.T)
    chosen = sine.reshape(SPACE, HALVES, CHUNKS, GROUP, 2, N).transpose(3, 0, 1, 2, 4, 5).reshape(GROUP, 64, N)
    anchor_y = left_table(chosen)
    anchor_x = left_table(sine.reshape(N // ROWS, ROWS, N))
    beside = np.zeros((2, SPACE, N))
    beside[0, 1:] = sine[15:-1:16]
    beside[1, :-1] = sine[16::16]
    beside = left_table(beside.reshape(16, N))
    line = eigen_values(N)
    plane = np.tile(line[:, None] + line[None, :], (1, 2)).astype(np.float32)
    along_y = np.repeat(line.reshape(SPACE, 8, 2), N, axis=2).astype(np.float32)
    return right, left, anchor_y, anchor_x, beside, plane, along_y


def two_parts(value, axis):
    high = value.astype(BF16)
    low = (value - high.astype(F32)).astype(BF16)
    return jnp.concatenate([high, low], axis=axis)


def along_rows(value, right_ref):
    made = jnp.dot(two_parts(value, 1), right_ref[...], preferred_element_type=F32)
    return made[:, :N] + made[:, N:]


def along_columns(left, value):
    made = jnp.dot(left, two_parts(value, 0), preferred_element_type=F32)
    half = made.shape[0] // 2
    return made[:half] + made[half:]


def kernel(
    forcing_ref, guess_ref, initial_ref, *refs,
):
    given, (
    solution_ref, residual_ref,
    cells, first_cells, gap_cells, sent, received, anchor_rows, anchor_sent, anchor_received, anchor,
    fine, weight, coarse, guess, begin, parts, change, change_before, scan_in, scan_out, error_before,
    back_sent, back_received, beside_sent, beside_received, beside_cells,
    load_sem, x_send, x_recv, plane_send, plane_recv, anchor_send, anchor_recv, shift_send, shift_recv,
    change_send, change_recv, scan_send, scan_recv, error_send, error_recv, back_send, back_recv,
    beside_send, beside_recv,
    table_sem, right_ref, left_ref, anchor_y_ref, anchor_x_ref, beside_ref, plane_ref, along_y_ref,
    ) = refs[:7], refs[7:]
    tables_here = (right_ref, left_ref, anchor_y_ref, anchor_x_ref, beside_ref, plane_ref, along_y_ref)
    t, s = lax.axis_index("tm"), lax.axis_index("space")
    after = lax.rem(t + 1, TM)
    right_of, left_of = lax.rem(s + 1, SPACE), lax.rem(s + SPACE - 1, SPACE)

    barrier = pltpu.get_barrier_semaphore()

    @pl.loop(0, TM - 1)
    def _(k):
        far = 1 + lax.rem(k + 15, TM - 1)
        pl.semaphore_signal(barrier, inc=1, device_id=(lax.rem(t + far, TM), s), device_id_type=MESH)

    for k in range(1, SPACE):
        pl.semaphore_signal(barrier, inc=1, device_id=(t, lax.rem(s + k, SPACE)), device_id_type=MESH)

    loads = [pltpu.make_async_copy(guess_ref.at[0], cells.at[0], load_sem.at[0])]
    loads += [pltpu.make_async_copy(forcing_ref.at[k], cells.at[k + 1], load_sem.at[k + 1]) for k in range(STEPS)]
    loads += [pltpu.make_async_copy(initial_ref, first_cells, load_sem.at[5])]
    loads[0].start()
    table_loads = [
        pltpu.make_async_copy(src, dst, table_sem.at[k]) for k, (src, dst) in enumerate(zip(given, tables_here))
    ]
    for load in table_loads[:2] + loads[1:] + table_loads[2:]:
        load.start()

    def remote(src, dst, send, recv, tm, space):
        return pltpu.make_async_remote_copy(
            src_ref=src, dst_ref=dst, send_sem=send, recv_sem=recv, device_id=(tm, space), device_id_type=MESH
        )

    def arrived(like, send, recv):
        remote(like, like, send, recv, after, s).wait_recv()

    def left_here(like, send, recv):
        remote(like, like, send, recv, after, s).wait_send()

    def over_columns(block):
        for pair in range(2):
            both = jnp.concatenate([block[(2 * pair + u) * N : (2 * pair + u + 1) * N] for u in range(2)], axis=1)
            yield pair, along_columns(left_ref[...], both)

    def put(slot, first, both):
        for u in range(2):
            one = both[:, u * N : (u + 1) * N].reshape(SPACE, HALVES, 8, N)
            for h in range(HALVES):
                sent[2 * slot + h, :, pl.ds(pl.multiple_of(8 * (first + u), 8), 8), :] = one[:, h]

    def to_modes(field, slot):
        @pl.loop(0, 4, unroll=True)
        def _(i):
            block = along_rows(cells[field, pl.ds(4 * i, 4)].reshape(4 * N, N), right_ref)
            for pair, both in over_columns(block):
                put(slot, 4 * i + 2 * pair, both)

    def middle_to_modes(slot):
        @pl.loop(0, 4, unroll=True)
        def _(i):
            here = gap_cells[pl.ds(4 * i + 1, 4)]
            bent = gap_cells[pl.ds(4 * i, 4)] + gap_cells[pl.ds(4 * i + 2, 4)] - 2.0 * here
            total = cells[2, pl.ds(4 * i, 4)] + cells[3, pl.ds(4 * i, 4)] + HALF_STEP * bent
            total = along_rows(total.reshape(4 * N, N), right_ref)
            here = along_rows(here.reshape(4 * N, N), right_ref)
            for (pair, both), (_, more) in zip(over_columns(total), over_columns(here)):
                put(slot, 4 * i + 2 * pair, both + (HALF_STEP * plane_ref[...]) * more)

    def exchange(slot, h):
        at = 2 * slot + h
        for k in range(1, SPACE):
            other = lax.rem(s + k, SPACE)
            remote(
                sent.at[at, other], received.at[at, pl.ds(pl.multiple_of(s * N, N), N)],
                x_send.at[at], x_recv.at[at], t, other,
            ).start()
        received[at, pl.ds(pl.multiple_of(s * N, N), N), :] = sent[at, s]

    def lines(at, pair):
        return jnp.concatenate(
            [received[at, pl.ds(2 * pair + u, N, stride=8), :] for u in range(2)], axis=1
        )

    def whole_lines(at):
        arrived(received.at[at, pl.ds(0, 7 * N)], x_send.at[at], x_recv.at[at])

    def pass_guess(h):
        whole_lines(h)
        for pair in range(PAIRS):
            guess[h, pair] = along_columns(left_ref[...], lines(h, pair))
        remote(guess.at[h], begin.at[h], shift_send.at[h], shift_recv.at[h], after, s).start()

    loads[0].wait()
    for load in table_loads:
        load.wait()
    to_modes(0, 0)
    loads[2].wait()
    loads[3].wait()
    gap_cells[pl.ds(1, 16)] = cells[2] - cells[3]
    pl.semaphore_wait(barrier, SPACE - 1 + TM - 1)
    exchange(0, 0)
    exchange(0, 1)
    planes = [
        remote(gap_cells.at[16], gap_cells.at[0], plane_send.at[0], plane_recv.at[0], t, right_of),
        remote(gap_cells.at[1], gap_cells.at[17], plane_send.at[1], plane_recv.at[1], t, left_of),
    ]
    for plane in planes:
        plane.start()
    loads[1].wait()
    to_modes(1, 1)
    exchange(1, 0)
    loads[4].wait()
    to_modes(4, 2)
    exchange(2, 0)
    pass_guess(0)
    for plane in planes:
        plane.wait_recv()
    gap_cells[0] = jnp.where(s == 0, jnp.zeros((N, N), F32), gap_cells[0])
    gap_cells[17] = jnp.where(s == SPACE - 1, jnp.zeros((N, N), F32), gap_cells[17])
    middle_to_modes(3)
    exchange(3, 0)
    pass_guess(1)

    loads[5].wait()
    column, block_of = lax.div(t, TM // GROUP), lax.rem(t, TM // GROUP)
    mine = pl.ds(pl.multiple_of(ROWS * block_of, ROWS), ROWS)

    @pl.loop(0, 4, unroll=True)
    def _(i):
        for pair in range(2):
            both = jnp.concatenate([first_cells[4 * i + 2 * pair + u] for u in range(2)], axis=1)
            both = along_columns(anchor_y_ref[column], both)
            both = jnp.concatenate([both[:, :N], both[:, N:]], axis=0)
            both = along_rows(both, right_ref)
            anchor_rows[pl.ds(pl.multiple_of(256 * i + 128 * pair, 128), 128), :] = both

    @pl.loop(0, SPACE)
    def _(other):
        for k in range(8):
            anchor_sent[other, pl.ds(16 * k, 16), :] = anchor_rows[pl.ds(8 * other + k, 16, stride=64), :]

    for k in range(1, SPACE):
        other = lax.rem(s + k, SPACE)
        remote(anchor_sent.at[other], anchor_received.at[s], anchor_send, anchor_recv, t, other).start()
    anchor_received[s] = anchor_sent[s]
    for slot in range(1, FIELDS):
        exchange(slot, 1)

    @pl.loop(0, HALVES * PAIRS)
    def _(i):
        spectrum = plane_ref[...] + along_y_ref[s, pl.ds(i, 1), :]
        inverse = 1.0 / (1.0 - HALF_STEP * spectrum)
        h, pair = lax.div(i, PAIRS), lax.rem(i, PAIRS)
        fine[h, pair] = (1.0 + HALF_STEP * spectrum) * inverse
        weight[h, pair] = TIME_STEP * inverse
        wide = STEPS * HALF_STEP
        coarse[h, pair] = (1.0 + wide * spectrum) / (1.0 - wide * spectrum)

    def pass_change(h, c):
        at, pairs = CHUNKS * h + c, pl.ds(GROUP * c, GROUP)
        remote(
            change.at[h, pairs], change_before.at[h, pairs], change_send.at[at], change_recv.at[at], after, s
        ).start()

    def relax(h):
        whole_lines(2 + h)

        @pl.loop(0, PAIRS, unroll=True)
        def _(pair):
            parts[0, h, pair] = along_columns(left_ref[...], lines(2 + h, pair)) * weight[h, pair]

        whole_lines(4 + h)

        @pl.loop(0, PAIRS, unroll=True)
        def _(pair):
            parts[2, h, pair] = along_columns(left_ref[...], lines(4 + h, pair)) * weight[h, pair]

        whole_lines(6 + h)
        arrived(begin.at[h], shift_send.at[h], shift_recv.at[h])
        for c in range(CHUNKS):

            @pl.loop(GROUP * c, GROUP * (c + 1), unroll=True)
            def _(pair):
                rate, scale = fine[h, pair], weight[h, pair]
                square = rate * rate
                third = along_columns(left_ref[...], lines(6 + h, pair)) * (scale * scale * (1.0 / TIME_STEP))
                third = third + square * parts[0, h, pair]
                parts[1, h, pair] = third
                value = parts[2, h, pair] + rate * third
                value = square * square * begin[h, pair] + value
                parts[2, h, pair] = value
                known = guess[h, pair]
                change[h, pair] = jnp.where(t == TM - 1, known, value - known)

            at = CHUNKS * h + c

            @pl.loop(0, TM - 1)
            def _(k):
                far = 1 + lax.rem(k + 15, TM - 1)
                other = lax.rem(t + far, TM)
                rows = pl.ds(pl.multiple_of(ROWS * lax.rem(other, TM // GROUP), ROWS), ROWS)
                remote(
                    change.at[h, GROUP * c + lax.div(other, TM // GROUP), rows], scan_in.at[at, t],
                    scan_send.at[at], scan_recv.at[at], other, s,
                ).start()

            scan_in[at, t] = change[h, GROUP * c + column, mine, :]
        pass_change(h, 0)

    def scan(h, c):
        at = CHUNKS * h + c
        arrived(scan_in.at[at, pl.ds(0, TM - 1)], scan_send.at[at], scan_recv.at[at])
        one = fine[h, GROUP * c + column, mine, :]
        square = one * one
        power, rate = square * square, coarse[h, GROUP * c + column, mine, :]
        first = anchor[at] - scan_in[at, TM - 1]
        scan_out[at, 0] = first

        def sweep(j, error):
            scan_out[at, j] = error
            return rate * error + power * scan_in[at, j - 1]

        scan_out[at, TM - 1] = lax.fori_loop(1, TM - 1, sweep, power * first)

        @pl.loop(0, TM - 1)
        def _(k):
            far = 1 + lax.rem(k + 15, TM - 1)
            other = lax.rem(t + far, TM)
            remote(
                scan_out.at[at, other], error_before.at[h, GROUP * c + column, mine],
                error_send.at[at], error_recv.at[at], other, s,
            ).start()

        error_before[h, GROUP * c + column, mine, :] = scan_out[at, t]

    def go_back(h, c):
        at, pairs = CHUNKS * h + c, pl.ds(GROUP * c, GROUP)
        arrived(change_before.at[h, pairs], change_send.at[at], change_recv.at[at])
        arrived(scan_out.at[at, pl.ds(0, TM - 1)], error_send.at[at], error_recv.at[at])

        @pl.loop(0, GROUP, unroll=True)
        def _(i):
            pair = GROUP * c + i
            came = error_before[h, pair]
            delta = jnp.where(t == 0, came, change_before[h, pair])
            error = jnp.where(t == 0, jnp.zeros_like(came), came)
            rate = fine[h, pair]
            square = rate * rate
            gap = square * square * delta
            for u in range(2):
                residual_ref[pl.ds(8 * h + 2 * pair + u, N, stride=16), :] = gap[:, u * N : (u + 1) * N]
            start = begin[h, pair] + (delta + error)
            first = rate * start + parts[0, h, pair]
            third = rate * square * start + parts[1, h, pair]
            last = parts[2, h, pair] + (gap + coarse[h, pair] * error)
            for k, point in enumerate((first, third, last)):
                point = along_columns(left_ref[...], point)
                for u in range(2):
                    rows = pl.ds(pl.multiple_of(32 * i + 16 * u, 16), 16)
                    back_sent[4 * k + at, :, rows, :] = point[:, u * N : (u + 1) * N].reshape(SPACE, 16, N)
            point = along_columns(beside_ref[...], first - third)
            for u in range(2):
                for side in range(2):
                    rows = pl.ds(4 * i + 2 * u + side, 8, stride=8)
                    beside_sent[at, rows, :] = point[8 * side : 8 * side + 8, u * N : (u + 1) * N]

        for k in range(BACK):
            slot = pl.ds(pl.multiple_of(256 * s + 64 * at, 64), 64)
            for hop in range(1, SPACE):
                other = lax.rem(s + hop, SPACE)
                remote(
                    back_sent.at[4 * k + at, other], back_received.at[k, slot],
                    back_send.at[4 * k + at], back_recv.at[4 * k + at], t, other,
                ).start()
            back_received[k, slot, :] = back_sent[4 * k + at, s]
            if k == 1:
                slot = pl.ds(pl.multiple_of(32 * s + 8 * at, 8), 8)
                for hop in range(1, SPACE):
                    other = lax.rem(s + hop, SPACE)
                    remote(
                        beside_sent.at[at, pl.ds(pl.multiple_of(8 * other, 8), 8)], beside_received.at[slot],
                        beside_send.at[at], beside_recv.at[at], t, other,
                    ).start()
                beside_received[slot, :] = beside_sent[at, pl.ds(pl.multiple_of(8 * s, 8), 8), :]

    relax(0)
    arrived(anchor_received.at[pl.ds(0, SPACE - 1)], anchor_send, anchor_recv)
    for at in range(HALVES * CHUNKS):
        both = jnp.concatenate(
            [anchor_received[:, pl.ds(32 * at + 16 * u, 16), :].reshape(N, N) for u in range(2)], axis=1
        )
        anchor[at] = along_columns(anchor_x_ref[block_of], both)
    scan(0, 0)
    pass_change(0, 1)
    scan(0, 1)
    relax(1)
    go_back(0, 0)
    go_back(0, 1)
    scan(1, 0)
    pass_change(1, 1)
    scan(1, 1)
    go_back(1, 0)
    go_back(1, 1)
    def back(k):
        for at in range(HALVES * CHUNKS):
            arrived(back_received.at[k, pl.ds(0, 7 * 64)], back_send.at[4 * k + at], back_recv.at[4 * k + at])

    def columns_at(k, x):
        return jnp.concatenate([back_received[k, pl.ds(x + u, N, stride=16), :] for u in range(2)], axis=1)

    def to_cells(four):
        pieces = []
        for both in four:
            both = along_columns(left_ref[...], both)
            pieces += [both[:, :N], both[:, N:]]
        return along_rows(jnp.concatenate(pieces, axis=0), right_ref)

    for k, step in ((0, 0), (1, 2)):
        back(k)

        @pl.loop(0, 4, unroll=True)
        def _(i):
            block = to_cells([columns_at(k, 4 * i + 2 * pair) for pair in range(2)])
            solution_ref[step, pl.ds(4 * i, 4)] = block.reshape(4, N, N)


    for at in range(HALVES * CHUNKS):
        arrived(beside_received.at[pl.ds(0, 7 * 8)], beside_send.at[at], beside_recv.at[at])
    both = jnp.concatenate([beside_received[pl.ds(side, N, stride=2), :] for side in range(2)], axis=1)
    beside_cells[pl.ds(0, 2)] = to_cells([both]).reshape(2, N, N)

    @pl.loop(0, 16)
    def _(x):
        beside_cells[x + 2] = solution_ref[0, x] - solution_ref[2, x]

    beside_cells[18] = beside_cells[1]
    beside_cells[1] = beside_cells[0]

    @pl.loop(0, 4, unroll=True)
    def _(i):
        four = [
            (columns_at(0, 4 * i + 2 * pair) - columns_at(1, 4 * i + 2 * pair)) * plane_ref[...]
            for pair in range(2)
        ]
        block = to_cells(four).reshape(4, N, N)
        planes = pl.ds(4 * i, 4)
        bent = beside_cells[pl.ds(4 * i + 1, 4)] + beside_cells[pl.ds(4 * i + 3, 4)]
        bent = bent - 2.0 * beside_cells[pl.ds(4 * i + 2, 4)] + block
        total = solution_ref[0, planes] + solution_ref[2, planes] + HALF_STEP * bent
        solution_ref[1, planes] = 0.5 * total + HALF_STEP * gap_cells[pl.ds(4 * i + 1, 4)]

    back(2)

    @pl.loop(0, 4, unroll=True)
    def _(i):
        block = to_cells([columns_at(2, 4 * i + 2 * pair) for pair in range(2)])
        solution_ref[3, pl.ds(4 * i, 4)] = block.reshape(4, N, N)


    for at in range(2 * FIELDS):
        left_here(received.at[at, pl.ds(0, 7 * N)], x_send.at[at], x_recv.at[at])
    for plane in planes:
        plane.wait_send()
    left_here(anchor_received.at[pl.ds(0, SPACE - 1)], anchor_send, anchor_recv)
    for h in range(HALVES):
        left_here(guess.at[h], shift_send.at[h], shift_recv.at[h])
    for at in range(HALVES * CHUNKS):
        left_here(change.at[0, pl.ds(0, GROUP)], change_send.at[at], change_recv.at[at])
        left_here(scan_in.at[at, pl.ds(0, TM - 1)], scan_send.at[at], scan_recv.at[at])
        left_here(scan_out.at[at, pl.ds(0, TM - 1)], error_send.at[at], error_recv.at[at])
        left_here(beside_received.at[pl.ds(0, 7 * 8)], beside_send.at[at], beside_recv.at[at])
    for at in range(BACK * HALVES * CHUNKS):
        left_here(back_received.at[0, pl.ds(0, 7 * 64)], back_send.at[at], back_recv.at[at])


def per_device(forcing, coarse_guess, initial):
    modal = (HALVES, PAIRS, N, 2 * N)
    quarters = HALVES * CHUNKS
    dma = pltpu.SemaphoreType.DMA
    vmem = pl.BlockSpec(memory_space=pltpu.VMEM)
    anywhere = pl.BlockSpec(memory_space=pltpu.HBM)
    given = tuple(jnp.asarray(one) for one in tables())
    out, gap = pl.pallas_call(
        kernel,
        out_shape=(
            jax.ShapeDtypeStruct((STEPS, 16, N, N), F32),
            jax.ShapeDtypeStruct((16 * N, N), F32),
        ),
        in_specs=[anywhere] * (3 + len(given)),
        out_specs=(vmem, vmem),
        scratch_shapes=[
            pltpu.VMEM((STEPS + 1, 16, N, N), F32),
            pltpu.VMEM((16, N, N), F32),
            pltpu.VMEM((18, N, N), F32),
            pltpu.VMEM((2 * FIELDS, SPACE, N, N), F32),
            pltpu.VMEM((2 * FIELDS, SPACE * N, N), F32),
            pltpu.VMEM((1024, N), F32),
            pltpu.VMEM((SPACE, N, N), F32),
            pltpu.VMEM((SPACE, N, N), F32),
            pltpu.VMEM((quarters, ROWS, 2 * N), F32),
            pltpu.VMEM(modal, F32),
            pltpu.VMEM(modal, F32),
            pltpu.VMEM(modal, F32),
            pltpu.VMEM(modal, F32),
            pltpu.VMEM(modal, F32),
            pltpu.VMEM((3,) + modal, F32),
            pltpu.VMEM(modal, F32),
            pltpu.VMEM(modal, F32),
            pltpu.VMEM((quarters, TM, ROWS, 2 * N), F32),
            pltpu.VMEM((quarters, TM, ROWS, 2 * N), F32),
            pltpu.VMEM(modal, F32),
            pltpu.VMEM((BACK * quarters, SPACE, 64, N), F32),
            pltpu.VMEM((BACK, 16 * N, N), F32),
            pltpu.VMEM((quarters, 64, N), F32),
            pltpu.VMEM((2 * N, N), F32),
            pltpu.VMEM((19, N, N), F32),
            dma((STEPS + 2,)),
            dma((2 * FIELDS,)),
            dma((2 * FIELDS,)),
            dma((2,)),
            dma((2,)),
            dma,
            dma,
            dma((HALVES,)),
            dma((HALVES,)),
            dma((quarters,)),
            dma((quarters,)),
            dma((quarters,)),
            dma((quarters,)),
            dma((quarters,)),
            dma((quarters,)),
            dma((BACK * quarters,)),
            dma((BACK * quarters,)),
            dma((quarters,)),
            dma((quarters,)),
            dma((len(given),)),
        ] + [pltpu.VMEM(one.shape, one.dtype) for one in given] + [
        ],
        compiler_params=pltpu.CompilerParams(
            collective_id=0, has_side_effects=True, vmem_limit_bytes=46 * 1024 * 1024
        ),
    )(*(pltpu.with_memory_space_constraint(one, pltpu.HBM) for one in (forcing, coarse_guess, initial) + given))
    return out, gap.reshape(1, N, 16, N)


def solution(mesh):
    in_specs = (P("tm", "space", None, None), P("tm", "space", None, None), P("space", None, None))
    out_specs = (P("tm", "space", None, None), P("tm", None, "space", None))
    return jax.shard_map(per_device, mesh=mesh, in_specs=in_specs, out_specs=out_specs, check_vma=False)
```

```python
import jax
import jax.numpy as jnp
import numpy as np
from jax import lax
from jax.experimental import pallas as pl
from jax.experimental.pallas import tpu as pltpu
from jax.sharding import PartitionSpec as P

MESH = pl.DeviceIdType.MESH
F32, BF16 = jnp.float32, jnp.bfloat16
N = 128
SPACE = 8
TM = 32
STEPS = 4
TIME_STEP = 0.5
HALVES = 2
PAIRS = 4
PIECES = HALVES * PAIRS
SHARE = TM // 2
ROWS = N // SHARE
FIELDS = 4
BACK = 3
HALF_STEP = 0.5 * TIME_STEP


def split_parts(table):
    high = table.astype(BF16)
    return high, (table - high.astype(np.float64)).astype(BF16)


def sine_table(length):
    ladder = np.arange(1, length + 1, dtype=np.float64)
    return np.sqrt(2.0 / (length + 1)) * np.sin(np.pi * ladder[:, None] * ladder[None, :] / (length + 1))


def eigen_values(length):
    ladder = np.arange(1, length + 1, dtype=np.float64)
    return -4.0 * np.sin(np.pi * ladder / (2 * (length + 1))) ** 2


def left_table(rows):
    high, low = split_parts(rows)
    return np.concatenate(
        [np.concatenate([high, high], axis=-1), np.concatenate([low, low], axis=-1)], axis=-2
    )


def tables():
    sine = sine_table(N)
    left = left_table(sine)
    right = np.ascontiguousarray(left.T)
    chosen = sine.reshape(SPACE, HALVES, PAIRS, 2, N).transpose(3, 0, 1, 2, 4).reshape(2, 64, N)
    anchor_y = left_table(chosen)
    anchor_x = left_table(sine.reshape(N // ROWS, ROWS, N))
    beside = np.zeros((2, SPACE, N))
    beside[0, 1:] = sine[15:-1:16]
    beside[1, :-1] = sine[16::16]
    beside = left_table(beside.reshape(16, N))
    line = eigen_values(N)
    plane = np.tile(line[:, None] + line[None, :], (1, 2)).astype(np.float32)
    along_y = np.repeat(line.reshape(SPACE, 8, 2), N, axis=2).astype(np.float32)
    return right, left, anchor_y, anchor_x, beside, plane, along_y


def two_parts(value, axis):
    high = value.astype(BF16)
    low = (value - high.astype(F32)).astype(BF16)
    return jnp.concatenate([high, low], axis=axis)


def along_rows(value, right_ref):
    made = jnp.dot(two_parts(value, 1), right_ref[...], preferred_element_type=F32)
    return made[:, :N] + made[:, N:]


def along_columns(left, value):
    made = jnp.dot(left, two_parts(value, 0), preferred_element_type=F32)
    half = made.shape[0] // 2
    return made[:half] + made[half:]


def kernel(
    forcing_ref, guess_ref, initial_ref, *refs,
):
    given, (
    solution_ref, residual_ref,
    cells, first_cells, gap_cells, sent, received, anchor_rows, anchor_sent, anchor_received, anchor,
    fine, weight, coarse, guess, begin, parts, change, change_before, scan_in, scan_out, error_before,
    back_sent, back_received, beside_sent, beside_received, beside_cells,
    load_sem, x_send, x_recv, plane_send, plane_recv, anchor_send, anchor_recv, shift_send, shift_recv,
    change_send, change_recv, scan_send, scan_recv, error_send, error_recv, back_send, back_recv,
    beside_send, beside_recv,
    entered, table_sem, right_ref, left_ref, anchor_y_ref, anchor_x_ref, beside_ref, plane_ref, along_y_ref,
    ) = refs[:7], refs[7:]
    tables_here = (right_ref, left_ref, anchor_y_ref, anchor_x_ref, beside_ref, plane_ref, along_y_ref)
    t, s = lax.axis_index("tm"), lax.axis_index("space")
    after = lax.rem(t + 1, TM)
    right_of, left_of = lax.rem(s + 1, SPACE), lax.rem(s + SPACE - 1, SPACE)

    barrier = pltpu.get_barrier_semaphore()

    for k in range(1, SPACE):
        pl.semaphore_signal(barrier, inc=1, device_id=(t, lax.rem(s + k, SPACE)), device_id_type=MESH)
    for other in (after, lax.rem(t + TM - 1, TM)):
        pl.semaphore_signal(barrier, inc=1, device_id=(other, s), device_id_type=MESH)

    def tell(r):
        for by in (1 << r, TM - (1 << r)):
            pl.semaphore_signal(entered.at[r], inc=1, device_id=(lax.rem(t + by, TM), s), device_id_type=MESH)

    def hear(r):
        pl.semaphore_wait(entered.at[r], 2)


    loads = [pltpu.make_async_copy(guess_ref.at[0], cells.at[0], load_sem.at[0])]
    loads += [pltpu.make_async_copy(forcing_ref.at[k], cells.at[k + 1], load_sem.at[k + 1]) for k in range(STEPS)]
    loads += [pltpu.make_async_copy(initial_ref, first_cells, load_sem.at[5])]
    loads[0].start()
    table_loads = [
        pltpu.make_async_copy(src, dst, table_sem.at[k]) for k, (src, dst) in enumerate(zip(given, tables_here))
    ]
    for load in table_loads[:2] + loads[1:] + table_loads[2:]:
        load.start()

    def remote(src, dst, send, recv, tm, space):
        return pltpu.make_async_remote_copy(
            src_ref=src, dst_ref=dst, send_sem=send, recv_sem=recv, device_id=(tm, space), device_id_type=MESH
        )

    def arrived(like, send, recv):
        remote(like, like, send, recv, after, s).wait_recv()

    def left_here(like, send, recv):
        remote(like, like, send, recv, after, s).wait_send()

    def over_columns(block):
        for pair in range(2):
            both = jnp.concatenate([block[(2 * pair + u) * N : (2 * pair + u + 1) * N] for u in range(2)], axis=1)
            yield pair, along_columns(left_ref[...], both)

    def put(slot, first, both):
        for u in range(2):
            one = both[:, u * N : (u + 1) * N].reshape(SPACE, HALVES, 8, N)
            for h in range(HALVES):
                sent[2 * slot + h, :, pl.ds(pl.multiple_of(8 * (first + u), 8), 8), :] = one[:, h]

    def to_modes(field, slot):
        @pl.loop(0, 4, unroll=True)
        def _(i):
            block = along_rows(cells[field, pl.ds(4 * i, 4)].reshape(4 * N, N), right_ref)
            for pair, both in over_columns(block):
                put(slot, 4 * i + 2 * pair, both)

    def middle_to_modes(slot):
        @pl.loop(0, 4, unroll=True)
        def _(i):
            here = gap_cells[pl.ds(4 * i + 1, 4)]
            bent = gap_cells[pl.ds(4 * i, 4)] + gap_cells[pl.ds(4 * i + 2, 4)] - 2.0 * here
            total = cells[2, pl.ds(4 * i, 4)] + cells[3, pl.ds(4 * i, 4)] + HALF_STEP * bent
            total = along_rows(total.reshape(4 * N, N), right_ref)
            here = along_rows(here.reshape(4 * N, N), right_ref)
            for (pair, both), (_, more) in zip(over_columns(total), over_columns(here)):
                put(slot, 4 * i + 2 * pair, both + (HALF_STEP * plane_ref[...]) * more)

    def exchange(slot, h):
        at = 2 * slot + h
        for k in range(1, SPACE):
            other = lax.rem(s + k, SPACE)
            remote(
                sent.at[at, other], received.at[at, pl.ds(pl.multiple_of(s * N, N), N)],
                x_send.at[at], x_recv.at[at], t, other,
            ).start()
        received[at, pl.ds(pl.multiple_of(s * N, N), N), :] = sent[at, s]

    def lines(at, pair):
        return jnp.concatenate(
            [received[at, pl.ds(2 * pair + u, N, stride=8), :] for u in range(2)], axis=1
        )

    def whole_lines(at):
        arrived(received.at[at, pl.ds(0, 7 * N)], x_send.at[at], x_recv.at[at])

    def pass_guess(h):
        whole_lines(h)
        for pair in range(PAIRS):
            guess[h, pair] = along_columns(left_ref[...], lines(h, pair))
        remote(guess.at[h], begin.at[h], shift_send.at[h], shift_recv.at[h], after, s).start()

    loads[0].wait()
    for load in table_loads:
        load.wait()
    to_modes(0, 0)
    loads[2].wait()
    loads[3].wait()
    gap_cells[pl.ds(1, 16)] = cells[2] - cells[3]
    pl.semaphore_wait(barrier, SPACE - 1 + 2)
    exchange(0, 0)
    exchange(0, 1)
    planes = [
        remote(gap_cells.at[16], gap_cells.at[0], plane_send.at[0], plane_recv.at[0], t, right_of),
        remote(gap_cells.at[1], gap_cells.at[17], plane_send.at[1], plane_recv.at[1], t, left_of),
    ]
    for plane in planes:
        plane.start()
    tell(0)
    loads[1].wait()
    to_modes(1, 1)
    exchange(1, 0)
    hear(0)
    tell(1)
    loads[4].wait()
    to_modes(4, 2)
    exchange(2, 0)
    hear(1)
    tell(2)
    pass_guess(0)
    for plane in planes:
        plane.wait_recv()
    gap_cells[0] = jnp.where(s == 0, jnp.zeros((N, N), F32), gap_cells[0])
    gap_cells[17] = jnp.where(s == SPACE - 1, jnp.zeros((N, N), F32), gap_cells[17])
    middle_to_modes(3)
    exchange(3, 0)
    hear(2)
    tell(3)
    pass_guess(1)
    hear(3)

    loads[5].wait()
    column, block_of = lax.div(t, SHARE), lax.rem(t, SHARE)
    mine = pl.ds(pl.multiple_of(ROWS * block_of, ROWS), ROWS)
    line = pl.ds(pl.multiple_of(N * column, N), N)

    @pl.loop(0, 4, unroll=True)
    def _(i):
        for pair in range(2):
            both = jnp.concatenate([first_cells[4 * i + 2 * pair + u] for u in range(2)], axis=1)
            both = along_columns(anchor_y_ref[column], both)
            both = jnp.concatenate([both[:, :N], both[:, N:]], axis=0)
            both = along_rows(both, right_ref)
            anchor_rows[pl.ds(pl.multiple_of(256 * i + 128 * pair, 128), 128), :] = both

    @pl.loop(0, SPACE)
    def _(other):
        for k in range(8):
            anchor_sent[other, pl.ds(16 * k, 16), :] = anchor_rows[pl.ds(8 * other + k, 16, stride=64), :]

    for k in range(1, SPACE):
        other = lax.rem(s + k, SPACE)
        remote(anchor_sent.at[other], anchor_received.at[s], anchor_send, anchor_recv, t, other).start()
    anchor_received[s] = anchor_sent[s]
    for slot in range(1, FIELDS):
        exchange(slot, 1)

    @pl.loop(0, HALVES * PAIRS)
    def _(i):
        spectrum = plane_ref[...] + along_y_ref[s, pl.ds(i, 1), :]
        inverse = 1.0 / (1.0 - HALF_STEP * spectrum)
        h, pair = lax.div(i, PAIRS), lax.rem(i, PAIRS)
        fine[h, pair] = (1.0 + HALF_STEP * spectrum) * inverse
        weight[h, pair] = TIME_STEP * inverse
        wide = STEPS * HALF_STEP
        coarse[h, pair] = (1.0 + wide * spectrum) / (1.0 - wide * spectrum)

    def pass_change(h, pair):
        at = PAIRS * h + pair
        remote(
            change.at[h, pair], change_before.at[h, pair], change_send.at[at], change_recv.at[at], after, s
        ).start()

    def relax(h):
        whole_lines(2 + h)

        @pl.loop(0, PAIRS, unroll=True)
        def _(pair):
            parts[0, h, pair] = along_columns(left_ref[...], lines(2 + h, pair)) * weight[h, pair]

        whole_lines(4 + h)

        @pl.loop(0, PAIRS, unroll=True)
        def _(pair):
            parts[2, h, pair] = along_columns(left_ref[...], lines(4 + h, pair)) * weight[h, pair]

        whole_lines(6 + h)
        arrived(begin.at[h], shift_send.at[h], shift_recv.at[h])
        for pair in range(PAIRS):
            rate, scale = fine[h, pair], weight[h, pair]
            square = rate * rate
            third = along_columns(left_ref[...], lines(6 + h, pair)) * (scale * scale * (1.0 / TIME_STEP))
            third = third + square * parts[0, h, pair]
            parts[1, h, pair] = third
            value = parts[2, h, pair] + rate * third
            value = square * square * begin[h, pair] + value
            parts[2, h, pair] = value
            known = guess[h, pair]
            change[h, pair] = jnp.where(t == TM - 1, known, value - known)
            at = PAIRS * h + pair

            @pl.loop(0, TM - 1)
            def _(k):
                far = 1 + lax.rem(k + 15, TM - 1)
                other = lax.rem(t + far, TM)
                rows = pl.ds(pl.multiple_of(ROWS * lax.rem(other, SHARE), ROWS), ROWS)
                lanes = pl.ds(pl.multiple_of(N * lax.div(other, SHARE), N), N)
                remote(
                    change.at[h, pair, rows, lanes], scan_in.at[at, t],
                    scan_send.at[at], scan_recv.at[at], other, s,
                ).start()

            scan_in[at, t] = change[h, pair, mine, line]
        pass_change(h, 0)

    def scan(h, pair):
        at = PAIRS * h + pair
        arrived(scan_in.at[at, pl.ds(0, TM - 1)], scan_send.at[at], scan_recv.at[at])
        one = fine[h, pair, mine, line]
        square = one * one
        power, rate = square * square, coarse[h, pair, mine, line]
        first = anchor[at] - scan_in[at, TM - 1]
        scan_out[at, 0] = first

        def sweep(j, error):
            scan_out[at, j] = error
            return rate * error + power * scan_in[at, j - 1]

        scan_out[at, TM - 1] = lax.fori_loop(1, TM - 1, sweep, power * first)

        @pl.loop(0, TM - 1)
        def _(k):
            far = 1 + lax.rem(k + 15, TM - 1)
            other = lax.rem(t + far, TM)
            remote(
                scan_out.at[at, other], error_before.at[h, pair, mine, line],
                error_send.at[at], error_recv.at[at], other, s,
            ).start()

        error_before[h, pair, mine, line] = scan_out[at, t]

    def go_back(h, pair):
        at = PAIRS * h + pair
        quarter, i = at // 2, pair % 2
        arrived(change_before.at[h, pair], change_send.at[at], change_recv.at[at])
        arrived(scan_out.at[at, pl.ds(0, TM - 1)], error_send.at[at], error_recv.at[at])
        came = error_before[h, pair]
        delta = jnp.where(t == 0, came, change_before[h, pair])
        error = jnp.where(t == 0, jnp.zeros_like(came), came)
        rate = fine[h, pair]
        square = rate * rate
        gap = square * square * delta
        for u in range(2):
            residual_ref[pl.ds(8 * h + 2 * pair + u, N, stride=16), :] = gap[:, u * N : (u + 1) * N]
        start = begin[h, pair] + (delta + error)
        first = rate * start + parts[0, h, pair]
        third = rate * square * start + parts[1, h, pair]
        last = parts[2, h, pair] + (gap + coarse[h, pair] * error)
        for k, point in enumerate((first, third, last)):
            point = along_columns(left_ref[...], point)
            for u in range(2):
                back_sent[PIECES * k + at, :, pl.ds(16 * u, 16), :] = point[:, u * N : (u + 1) * N].reshape(SPACE, 16, N)
        point = along_columns(beside_ref[...], first - third)
        for u in range(2):
            for side in range(2):
                rows = pl.ds(4 * i + 2 * u + side, 8, stride=8)
                beside_sent[quarter, rows, :] = point[8 * side : 8 * side + 8, u * N : (u + 1) * N]

        for k in range(BACK):
            slot = pl.ds(pl.multiple_of(256 * s + 32 * at, 32), 32)
            for hop in range(1, SPACE):
                other = lax.rem(s + hop, SPACE)
                remote(
                    back_sent.at[PIECES * k + at, other], back_received.at[k, slot],
                    back_send.at[PIECES * k + at], back_recv.at[PIECES * k + at], t, other,
                ).start()
            back_received[k, slot, :] = back_sent[PIECES * k + at, s]
            if k == 1 and i == 1:
                slot = pl.ds(pl.multiple_of(32 * s + 8 * quarter, 8), 8)
                for hop in range(1, SPACE):
                    other = lax.rem(s + hop, SPACE)
                    remote(
                        beside_sent.at[quarter, pl.ds(pl.multiple_of(8 * other, 8), 8)], beside_received.at[slot],
                        beside_send.at[quarter], beside_recv.at[quarter], t, other,
                    ).start()
                beside_received[slot, :] = beside_sent[quarter, pl.ds(pl.multiple_of(8 * s, 8), 8), :]

    relax(0)
    arrived(anchor_received.at[pl.ds(0, SPACE - 1)], anchor_send, anchor_recv)
    for at in range(PIECES):
        both = anchor_received[:, pl.ds(16 * at, 16), :].reshape(N, N)
        anchor[at] = along_columns(anchor_x_ref[block_of], both)
    for pair in range(PAIRS):
        scan(0, pair)
        if pair + 2 < PAIRS:
            pass_change(0, pair + 1)
    pass_change(0, PAIRS - 1)
    relax(1)
    for pair in range(PAIRS):
        go_back(0, pair)
    for pair in range(PAIRS):
        scan(1, pair)
        if pair + 2 < PAIRS:
            pass_change(1, pair + 1)
    pass_change(1, PAIRS - 1)
    for pair in range(PAIRS):
        go_back(1, pair)

    for at in range(2 * FIELDS):
        left_here(received.at[at, pl.ds(0, 7 * N)], x_send.at[at], x_recv.at[at])
    for plane in planes:
        plane.wait_send()
    left_here(anchor_received.at[pl.ds(0, SPACE - 1)], anchor_send, anchor_recv)
    for h in range(HALVES):
        left_here(guess.at[h], shift_send.at[h], shift_recv.at[h])
    for at in range(PIECES):
        left_here(change.at[0, 0], change_send.at[at], change_recv.at[at])
        left_here(scan_in.at[at, pl.ds(0, TM - 1)], scan_send.at[at], scan_recv.at[at])
        left_here(scan_out.at[at, pl.ds(0, TM - 1)], error_send.at[at], error_recv.at[at])
    for k in range(BACK):
        for at in range(PIECES * k, PIECES * (k + 1) - 1):
            left_here(back_received.at[0, pl.ds(0, 7 * 32)], back_send.at[at], back_recv.at[at])

    def back(k):
        for at in range(PIECES):
            here = PIECES * k + at
            arrived(back_received.at[k, pl.ds(0, 7 * 32)], back_send.at[here], back_recv.at[here])

    def columns_at(k, x):
        return jnp.concatenate([back_received[k, pl.ds(x + u, N, stride=16), :] for u in range(2)], axis=1)

    def to_cells(four):
        pieces = []
        for both in four:
            both = along_columns(left_ref[...], both)
            pieces += [both[:, :N], both[:, N:]]
        return along_rows(jnp.concatenate(pieces, axis=0), right_ref)

    for k, step in ((0, 0), (1, 2)):
        back(k)

        @pl.loop(0, 4, unroll=True)
        def _(i):
            block = to_cells([columns_at(k, 4 * i + 2 * pair) for pair in range(2)])
            solution_ref[step, pl.ds(4 * i, 4)] = block.reshape(4, N, N)


    for at in range(PIECES // 2):
        arrived(beside_received.at[pl.ds(0, 7 * 8)], beside_send.at[at], beside_recv.at[at])
    both = jnp.concatenate([beside_received[pl.ds(side, N, stride=2), :] for side in range(2)], axis=1)
    beside_cells[pl.ds(0, 2)] = to_cells([both]).reshape(2, N, N)

    @pl.loop(0, 16)
    def _(x):
        beside_cells[x + 2] = solution_ref[0, x] - solution_ref[2, x]

    beside_cells[18] = beside_cells[1]
    beside_cells[1] = beside_cells[0]

    @pl.loop(0, 4, unroll=True)
    def _(i):
        four = [
            (columns_at(0, 4 * i + 2 * pair) - columns_at(1, 4 * i + 2 * pair)) * plane_ref[...]
            for pair in range(2)
        ]
        block = to_cells(four).reshape(4, N, N)
        planes = pl.ds(4 * i, 4)
        bent = beside_cells[pl.ds(4 * i + 1, 4)] + beside_cells[pl.ds(4 * i + 3, 4)]
        bent = bent - 2.0 * beside_cells[pl.ds(4 * i + 2, 4)] + block
        total = solution_ref[0, planes] + solution_ref[2, planes] + HALF_STEP * bent
        solution_ref[1, planes] = 0.5 * total + HALF_STEP * gap_cells[pl.ds(4 * i + 1, 4)]

    back(2)

    @pl.loop(0, 4, unroll=True)
    def _(i):
        block = to_cells([columns_at(2, 4 * i + 2 * pair) for pair in range(2)])
        solution_ref[3, pl.ds(4 * i, 4)] = block.reshape(4, N, N)


    for at in range(PIECES // 2):
        left_here(beside_received.at[pl.ds(0, 7 * 8)], beside_send.at[at], beside_recv.at[at])
    for k in range(BACK):
        at = PIECES * (k + 1) - 1
        left_here(back_received.at[0, pl.ds(0, 7 * 32)], back_send.at[at], back_recv.at[at])

def per_device(forcing, coarse_guess, initial):
    modal = (HALVES, PAIRS, N, 2 * N)
    quarters = PIECES // 2
    dma = pltpu.SemaphoreType.DMA
    vmem = pl.BlockSpec(memory_space=pltpu.VMEM)
    anywhere = pl.BlockSpec(memory_space=pltpu.HBM)
    given = tuple(jnp.asarray(one) for one in tables())
    out, gap = pl.pallas_call(
        kernel,
        out_shape=(
            jax.ShapeDtypeStruct((STEPS, 16, N, N), F32),
            jax.ShapeDtypeStruct((16 * N, N), F32),
        ),
        in_specs=[anywhere] * (3 + len(given)),
        out_specs=(vmem, vmem),
        scratch_shapes=[
            pltpu.VMEM((STEPS + 1, 16, N, N), F32),
            pltpu.VMEM((16, N, N), F32),
            pltpu.VMEM((18, N, N), F32),
            pltpu.VMEM((2 * FIELDS, SPACE, N, N), F32),
            pltpu.VMEM((2 * FIELDS, SPACE * N, N), F32),
            pltpu.VMEM((1024, N), F32),
            pltpu.VMEM((SPACE, N, N), F32),
            pltpu.VMEM((SPACE, N, N), F32),
            pltpu.VMEM((PIECES, ROWS, N), F32),
            pltpu.VMEM(modal, F32),
            pltpu.VMEM(modal, F32),
            pltpu.VMEM(modal, F32),
            pltpu.VMEM(modal, F32),
            pltpu.VMEM(modal, F32),
            pltpu.VMEM((3,) + modal, F32),
            pltpu.VMEM(modal, F32),
            pltpu.VMEM(modal, F32),
            pltpu.VMEM((PIECES, TM, ROWS, N), F32),
            pltpu.VMEM((PIECES, TM, ROWS, N), F32),
            pltpu.VMEM(modal, F32),
            pltpu.VMEM((BACK * PIECES, SPACE, 32, N), F32),
            pltpu.VMEM((BACK, 16 * N, N), F32),
            pltpu.VMEM((quarters, 64, N), F32),
            pltpu.VMEM((2 * N, N), F32),
            pltpu.VMEM((19, N, N), F32),
            dma((STEPS + 2,)),
            dma((2 * FIELDS,)),
            dma((2 * FIELDS,)),
            dma((2,)),
            dma((2,)),
            dma,
            dma,
            dma((HALVES,)),
            dma((HALVES,)),
            dma((PIECES,)),
            dma((PIECES,)),
            dma((PIECES,)),
            dma((PIECES,)),
            dma((PIECES,)),
            dma((PIECES,)),
            dma((BACK * PIECES,)),
            dma((BACK * PIECES,)),
            dma((quarters,)),
            dma((quarters,)),
            pltpu.SemaphoreType.REGULAR((4,)),
            dma((len(given),)),
        ] + [pltpu.VMEM(one.shape, one.dtype) for one in given] + [
        ],
        compiler_params=pltpu.CompilerParams(
            collective_id=0, has_side_effects=True, vmem_limit_bytes=46 * 1024 * 1024
        ),
    )(*(pltpu.with_memory_space_constraint(one, pltpu.HBM) for one in (forcing, coarse_guess, initial) + given))
    return out, gap.reshape(1, N, 16, N)


def solution(mesh):
    in_specs = (P("tm", "space", None, None), P("tm", "space", None, None), P("space", None, None))
    out_specs = (P("tm", "space", None, None), P("tm", None, "space", None))
    return jax.shard_map(per_device, mesh=mesh, in_specs=in_specs, out_specs=out_specs, check_vma=False)
```

```python
import jax
import jax.numpy as jnp
import numpy as np
from jax import lax
from jax.experimental import pallas as pl
from jax.experimental.pallas import tpu as pltpu
from jax.sharding import PartitionSpec as P

MESH = pl.DeviceIdType.MESH
F32, BF16 = jnp.float32, jnp.bfloat16
N = 128
SPACE = 8
TM = 32
STEPS = 4
TIME_STEP = 0.5
HALVES = 2
PAIRS = 4
PIECES = HALVES * PAIRS
SHARE = TM // 2
ROWS = N // SHARE
FIELDS = 4
BACK = 3
HALF_STEP = 0.5 * TIME_STEP


def split_parts(table):
    high = table.astype(BF16)
    return high, (table - high.astype(np.float64)).astype(BF16)


def sine_table(length):
    ladder = np.arange(1, length + 1, dtype=np.float64)
    return np.sqrt(2.0 / (length + 1)) * np.sin(np.pi * ladder[:, None] * ladder[None, :] / (length + 1))


def eigen_values(length):
    ladder = np.arange(1, length + 1, dtype=np.float64)
    return -4.0 * np.sin(np.pi * ladder / (2 * (length + 1))) ** 2


def left_table(rows):
    high, low = split_parts(rows)
    return np.concatenate(
        [np.concatenate([high, high], axis=-1), np.concatenate([low, low], axis=-1)], axis=-2
    )


def tables():
    sine = sine_table(N)
    left = left_table(sine)
    right = np.ascontiguousarray(left.T)
    chosen = sine.reshape(SPACE, HALVES, PAIRS, 2, N).transpose(3, 0, 1, 2, 4).reshape(2, 64, N)
    anchor_y = left_table(chosen)
    anchor_x = left_table(sine.reshape(N // ROWS, ROWS, N))
    beside = np.zeros((2, SPACE, N))
    beside[0, 1:] = sine[15:-1:16]
    beside[1, :-1] = sine[16::16]
    beside = left_table(beside.reshape(16, N))
    line = eigen_values(N)
    plane = np.tile(line[:, None] + line[None, :], (1, 2)).astype(np.float32)
    along_y = np.repeat(line.reshape(SPACE, 8, 2), N, axis=2).astype(np.float32)
    return right, left, anchor_y, anchor_x, beside, plane, along_y


def two_parts(value, axis):
    high = value.astype(BF16)
    low = (value - high.astype(F32)).astype(BF16)
    return jnp.concatenate([high, low], axis=axis)


def along_rows(value, right_ref):
    made = jnp.dot(two_parts(value, 1), right_ref[...], preferred_element_type=F32)
    return made[:, :N] + made[:, N:]


def along_columns(left, value):
    made = jnp.dot(left, two_parts(value, 0), preferred_element_type=F32)
    half = made.shape[0] // 2
    return made[:half] + made[half:]


def kernel(
    forcing_ref, guess_ref, initial_ref, *refs,
):
    given, (
    solution_ref, residual_ref,
    cells, first_cells, gap_cells, sent, received, anchor_rows, anchor_sent, anchor_received, anchor,
    fine, weight, coarse, guess, begin, parts, change, change_before, scan_in, scan_out, error_before,
    back_sent, back_received, beside_sent, beside_received, beside_cells,
    load_sem, x_send, x_recv, plane_send, plane_recv, anchor_send, anchor_recv, shift_send, shift_recv,
    change_send, change_recv, scan_send, scan_recv, error_send, error_recv, back_send, back_recv,
    beside_send, beside_recv,
    entered, table_sem, right_ref, left_ref, anchor_y_ref, anchor_x_ref, beside_ref, plane_ref, along_y_ref,
    ) = refs[:7], refs[7:]
    tables_here = (right_ref, left_ref, anchor_y_ref, anchor_x_ref, beside_ref, plane_ref, along_y_ref)
    t, s = lax.axis_index("tm"), lax.axis_index("space")
    after = lax.rem(t + 1, TM)
    right_of, left_of = lax.rem(s + 1, SPACE), lax.rem(s + SPACE - 1, SPACE)

    barrier = pltpu.get_barrier_semaphore()

    for k in range(1, SPACE):
        pl.semaphore_signal(barrier, inc=1, device_id=(t, lax.rem(s + k, SPACE)), device_id_type=MESH)
    for other in (after, lax.rem(t + TM - 1, TM)):
        pl.semaphore_signal(barrier, inc=1, device_id=(other, s), device_id_type=MESH)

    def tell(r):
        for by in (1 << r, TM - (1 << r)):
            pl.semaphore_signal(entered.at[r], inc=1, device_id=(lax.rem(t + by, TM), s), device_id_type=MESH)

    def hear(r):
        pl.semaphore_wait(entered.at[r], 2)


    loads = [pltpu.make_async_copy(guess_ref.at[0], cells.at[0], load_sem.at[0])]
    loads += [pltpu.make_async_copy(forcing_ref.at[k], cells.at[k + 1], load_sem.at[k + 1]) for k in range(STEPS)]
    loads += [pltpu.make_async_copy(initial_ref, first_cells, load_sem.at[5])]
    loads[0].start()
    table_loads = [
        pltpu.make_async_copy(src, dst, table_sem.at[k]) for k, (src, dst) in enumerate(zip(given, tables_here))
    ]
    for load in table_loads[:2] + loads[1:] + table_loads[2:]:
        load.start()

    def remote(src, dst, send, recv, tm, space):
        return pltpu.make_async_remote_copy(
            src_ref=src, dst_ref=dst, send_sem=send, recv_sem=recv, device_id=(tm, space), device_id_type=MESH
        )

    def arrived(like, send, recv):
        remote(like, like, send, recv, after, s).wait_recv()

    def left_here(like, send, recv):
        remote(like, like, send, recv, after, s).wait_send()

    def over_columns(block):
        for pair in range(2):
            both = jnp.concatenate([block[(2 * pair + u) * N : (2 * pair + u + 1) * N] for u in range(2)], axis=1)
            yield pair, along_columns(left_ref[...], both)

    def put(slot, first, both):
        for u in range(2):
            one = both[:, u * N : (u + 1) * N].reshape(SPACE, HALVES, 8, N)
            for h in range(HALVES):
                sent[2 * slot + h, :, pl.ds(pl.multiple_of(8 * (first + u), 8), 8), :] = one[:, h]

    def to_modes(field, slot):
        @pl.loop(0, 4, unroll=True)
        def _(i):
            block = along_rows(cells[field, pl.ds(4 * i, 4)].reshape(4 * N, N), right_ref)
            for pair, both in over_columns(block):
                put(slot, 4 * i + 2 * pair, both)

    def middle_to_modes(slot):
        @pl.loop(0, 4, unroll=True)
        def _(i):
            here = gap_cells[pl.ds(4 * i + 1, 4)]
            bent = gap_cells[pl.ds(4 * i, 4)] + gap_cells[pl.ds(4 * i + 2, 4)] - 2.0 * here
            total = cells[2, pl.ds(4 * i, 4)] + cells[3, pl.ds(4 * i, 4)] + HALF_STEP * bent
            total = along_rows(total.reshape(4 * N, N), right_ref)
            here = along_rows(here.reshape(4 * N, N), right_ref)
            for (pair, both), (_, more) in zip(over_columns(total), over_columns(here)):
                put(slot, 4 * i + 2 * pair, both + (HALF_STEP * plane_ref[...]) * more)

    def exchange(slot, h):
        at = 2 * slot + h
        for k in range(1, SPACE):
            other = lax.rem(s + k, SPACE)
            remote(
                sent.at[at, other], received.at[at, pl.ds(pl.multiple_of(s * N, N), N)],
                x_send.at[at], x_recv.at[at], t, other,
            ).start()
        received[at, pl.ds(pl.multiple_of(s * N, N), N), :] = sent[at, s]

    def lines(at, pair):
        return jnp.concatenate(
            [received[at, pl.ds(2 * pair + u, N, stride=8), :] for u in range(2)], axis=1
        )

    def whole_lines(at):
        arrived(received.at[at, pl.ds(0, 7 * N)], x_send.at[at], x_recv.at[at])

    def pass_guess(h):
        whole_lines(h)
        for pair in range(PAIRS):
            guess[h, pair] = along_columns(left_ref[...], lines(h, pair))
        remote(guess.at[h], begin.at[h], shift_send.at[h], shift_recv.at[h], after, s).start()

    loads[0].wait()
    for load in table_loads:
        load.wait()
    to_modes(0, 0)
    loads[2].wait()
    loads[3].wait()
    gap_cells[pl.ds(1, 16)] = cells[2] - cells[3]
    pl.semaphore_wait(barrier, SPACE - 1 + 2)
    exchange(0, 0)
    exchange(0, 1)
    planes = [
        remote(gap_cells.at[16], gap_cells.at[0], plane_send.at[0], plane_recv.at[0], t, right_of),
        remote(gap_cells.at[1], gap_cells.at[17], plane_send.at[1], plane_recv.at[1], t, left_of),
    ]
    for plane in planes:
        plane.start()
    tell(0)
    loads[1].wait()
    to_modes(1, 1)
    exchange(1, 0)
    hear(0)
    tell(1)
    loads[4].wait()
    to_modes(4, 2)
    exchange(2, 0)
    hear(1)
    tell(2)
    pass_guess(0)
    for plane in planes:
        plane.wait_recv()
    gap_cells[0] = jnp.where(s == 0, jnp.zeros((N, N), F32), gap_cells[0])
    gap_cells[17] = jnp.where(s == SPACE - 1, jnp.zeros((N, N), F32), gap_cells[17])
    middle_to_modes(3)
    exchange(3, 0)
    hear(2)
    tell(3)
    pass_guess(1)
    hear(3)

    loads[5].wait()
    column, block_of = lax.div(t, SHARE), lax.rem(t, SHARE)
    mine = pl.ds(pl.multiple_of(ROWS * block_of, ROWS), ROWS)
    line = pl.ds(pl.multiple_of(N * column, N), N)

    @pl.loop(0, 4, unroll=True)
    def _(i):
        for pair in range(2):
            both = jnp.concatenate([first_cells[4 * i + 2 * pair + u] for u in range(2)], axis=1)
            both = along_columns(anchor_y_ref[column], both)
            both = jnp.concatenate([both[:, :N], both[:, N:]], axis=0)
            both = along_rows(both, right_ref)
            anchor_rows[pl.ds(pl.multiple_of(256 * i + 128 * pair, 128), 128), :] = both

    @pl.loop(0, SPACE)
    def _(other):
        for k in range(8):
            anchor_sent[other, pl.ds(16 * k, 16), :] = anchor_rows[pl.ds(8 * other + k, 16, stride=64), :]

    for k in range(1, SPACE):
        other = lax.rem(s + k, SPACE)
        remote(anchor_sent.at[other], anchor_received.at[s], anchor_send, anchor_recv, t, other).start()
    anchor_received[s] = anchor_sent[s]
    for slot in range(1, FIELDS):
        exchange(slot, 1)

    @pl.loop(0, HALVES * PAIRS)
    def _(i):
        spectrum = plane_ref[...] + along_y_ref[s, pl.ds(i, 1), :]
        inverse = 1.0 / (1.0 - HALF_STEP * spectrum)
        h, pair = lax.div(i, PAIRS), lax.rem(i, PAIRS)
        fine[h, pair] = (1.0 + HALF_STEP * spectrum) * inverse
        weight[h, pair] = TIME_STEP * inverse
        wide = STEPS * HALF_STEP
        coarse[h, pair] = (1.0 + wide * spectrum) / (1.0 - wide * spectrum)

    def pass_change(h, pair):
        at = PAIRS * h + pair
        remote(
            change.at[h, pair], change_before.at[h, pair], change_send.at[at], change_recv.at[at], after, s
        ).start()

    def relax(h):
        whole_lines(2 + h)

        @pl.loop(0, PAIRS, unroll=True)
        def _(pair):
            parts[0, h, pair] = along_columns(left_ref[...], lines(2 + h, pair)) * weight[h, pair]

        whole_lines(4 + h)

        @pl.loop(0, PAIRS, unroll=True)
        def _(pair):
            parts[2, h, pair] = along_columns(left_ref[...], lines(4 + h, pair)) * weight[h, pair]

        whole_lines(6 + h)
        arrived(begin.at[h], shift_send.at[h], shift_recv.at[h])
        for pair in range(PAIRS):
            rate, scale = fine[h, pair], weight[h, pair]
            square = rate * rate
            third = along_columns(left_ref[...], lines(6 + h, pair)) * (scale * scale * (1.0 / TIME_STEP))
            third = third + square * parts[0, h, pair]
            parts[1, h, pair] = third
            value = parts[2, h, pair] + rate * third
            value = square * square * begin[h, pair] + value
            parts[2, h, pair] = value
            known = guess[h, pair]
            change[h, pair] = jnp.where(t == TM - 1, known, value - known)
            at = PAIRS * h + pair

            @pl.loop(0, TM - 1)
            def _(k):
                far = 1 + lax.rem(k + 15, TM - 1)
                other = lax.rem(t + far, TM)
                rows = pl.ds(pl.multiple_of(ROWS * lax.rem(other, SHARE), ROWS), ROWS)
                lanes = pl.ds(pl.multiple_of(N * lax.div(other, SHARE), N), N)
                remote(
                    change.at[h, pair, rows, lanes], scan_in.at[at, t],
                    scan_send.at[at], scan_recv.at[at], other, s,
                ).start()

            scan_in[at, t] = change[h, pair, mine, line]
        pass_change(h, 0)

    def scan(h, pair):
        at = PAIRS * h + pair
        arrived(scan_in.at[at, pl.ds(0, TM - 1)], scan_send.at[at], scan_recv.at[at])
        one = fine[h, pair, mine, line]
        square = one * one
        power, rate = square * square, coarse[h, pair, mine, line]
        first = anchor[at] - scan_in[at, TM - 1]
        scan_out[at, 0] = first

        def sweep(j, error):
            scan_out[at, j] = error
            return rate * error + power * scan_in[at, j - 1]

        scan_out[at, TM - 1] = lax.fori_loop(1, TM - 1, sweep, power * first)

        @pl.loop(0, TM - 1)
        def _(k):
            far = 1 + lax.rem(k + 15, TM - 1)
            other = lax.rem(t + far, TM)
            remote(
                scan_out.at[at, other], error_before.at[h, pair, mine, line],
                error_send.at[at], error_recv.at[at], other, s,
            ).start()

        error_before[h, pair, mine, line] = scan_out[at, t]

    def go_back(h, pair):
        at = PAIRS * h + pair
        quarter, i = at // 2, pair % 2
        arrived(change_before.at[h, pair], change_send.at[at], change_recv.at[at])
        arrived(scan_out.at[at, pl.ds(0, TM - 1)], error_send.at[at], error_recv.at[at])
        came = error_before[h, pair]
        delta = jnp.where(t == 0, came, change_before[h, pair])
        error = jnp.where(t == 0, jnp.zeros_like(came), came)
        rate = fine[h, pair]
        square = rate * rate
        gap = square * square * delta
        for u in range(2):
            residual_ref[pl.ds(8 * h + 2 * pair + u, N, stride=16), :] = gap[:, u * N : (u + 1) * N]
        start = begin[h, pair] + (delta + error)
        first = rate * start + parts[0, h, pair]
        third = rate * square * start + parts[1, h, pair]
        last = parts[2, h, pair] + (gap + coarse[h, pair] * error)
        for k, point in enumerate((first, third, last)):
            point = along_columns(left_ref[...], point)
            for u in range(2):
                back_sent[PIECES * k + at, :, pl.ds(16 * u, 16), :] = point[:, u * N : (u + 1) * N].reshape(SPACE, 16, N)
        point = along_columns(beside_ref[...], first - third)
        for u in range(2):
            for side in range(2):
                rows = pl.ds(4 * i + 2 * u + side, 8, stride=8)
                beside_sent[quarter, rows, :] = point[8 * side : 8 * side + 8, u * N : (u + 1) * N]

        for k in range(BACK):
            slot = pl.ds(pl.multiple_of(256 * s + 32 * at, 32), 32)
            for hop in range(1, SPACE):
                other = lax.rem(s + hop, SPACE)
                remote(
                    back_sent.at[PIECES * k + at, other], back_received.at[k, slot],
                    back_send.at[PIECES * k + at], back_recv.at[PIECES * k + at], t, other,
                ).start()
            back_received[k, slot, :] = back_sent[PIECES * k + at, s]
            if k == 1 and i == 1:
                slot = pl.ds(pl.multiple_of(32 * s + 8 * quarter, 8), 8)
                for hop in range(1, SPACE):
                    other = lax.rem(s + hop, SPACE)
                    remote(
                        beside_sent.at[quarter, pl.ds(pl.multiple_of(8 * other, 8), 8)], beside_received.at[slot],
                        beside_send.at[quarter], beside_recv.at[quarter], t, other,
                    ).start()
                beside_received[slot, :] = beside_sent[quarter, pl.ds(pl.multiple_of(8 * s, 8), 8), :]

    relax(0)
    arrived(anchor_received.at[pl.ds(0, SPACE - 1)], anchor_send, anchor_recv)
    for at in range(PIECES):
        both = anchor_received[:, pl.ds(16 * at, 16), :].reshape(N, N)
        anchor[at] = along_columns(anchor_x_ref[block_of], both)
    for pair in range(PAIRS):
        scan(0, pair)
        if pair + 2 < PAIRS:
            pass_change(0, pair + 1)
    pass_change(0, PAIRS - 1)
    relax(1)
    for pair in range(PAIRS):
        go_back(0, pair)
    for pair in range(PAIRS):
        scan(1, pair)
        if pair + 2 < PAIRS:
            pass_change(1, pair + 1)
    pass_change(1, PAIRS - 1)
    def back(k, pieces):
        for at in pieces:
            here = PIECES * k + at
            arrived(back_received.at[k, pl.ds(0, 7 * 32)], back_send.at[here], back_recv.at[here])

    def middle_rows(first, count):
        for other in range(SPACE):
            rows = pl.ds(256 * other + 32 * first, 32 * count)
            gap = (back_received[0, rows, :] - back_received[1, rows, :]).reshape(2 * count, 16, N)
            scale = plane_ref[pl.ds(16 * other + 2 * first, 2 * count), pl.ds(0, N)]
            back_received[BACK, rows, :] = (gap * scale[:, None, :]).reshape(32 * count, N)

    def rows_to_cells(k, first, count):
        parts_of = [pl.ds(256 * other + 32 * first, 32 * count) for other in range(SPACE)]
        for four in (parts_of[:4], parts_of[4:]):
            block = jnp.concatenate([back_received[k, rows, :] for rows in four], axis=0)
            block = along_rows(block, right_ref)
            for n, rows in enumerate(four):
                back_received[k, rows, :] = block[32 * count * n : 32 * count * (n + 1)]

    for pair in range(PAIRS - 1):
        go_back(1, pair)
    early, late = range(5), range(5, PIECES)
    for k in range(BACK):
        back(k, early)
    middle_rows(0, 5)
    for k in range(BACK + 1):
        rows_to_cells(k, 0, 5)
    go_back(1, PAIRS - 1)

    for at in range(2 * FIELDS):
        left_here(received.at[at, pl.ds(0, 7 * N)], x_send.at[at], x_recv.at[at])
    for plane in planes:
        plane.wait_send()
    left_here(anchor_received.at[pl.ds(0, SPACE - 1)], anchor_send, anchor_recv)
    for h in range(HALVES):
        left_here(guess.at[h], shift_send.at[h], shift_recv.at[h])
    for at in range(PIECES):
        left_here(change.at[0, 0], change_send.at[at], change_recv.at[at])
        left_here(scan_in.at[at, pl.ds(0, TM - 1)], scan_send.at[at], scan_recv.at[at])
        left_here(scan_out.at[at, pl.ds(0, TM - 1)], error_send.at[at], error_recv.at[at])
    for k in range(BACK):
        for at in range(PIECES * k, PIECES * (k + 1) - 1):
            left_here(back_received.at[0, pl.ds(0, 7 * 32)], back_send.at[at], back_recv.at[at])

    def columns_at(k, x):
        return jnp.concatenate([back_received[k, pl.ds(x + u, N, stride=16), :] for u in range(2)], axis=1)

    def to_cells(k, x):
        both = along_columns(left_ref[...], columns_at(k, x))
        return both[:, :N], both[:, N:]

    back(0, late)
    back(1, late)
    middle_rows(5, 3)
    for k, step in ((0, 0), (1, 2)):
        rows_to_cells(k, 5, 3)

        @pl.loop(0, 8, unroll=True)
        def _(i):
            for u, one in enumerate(to_cells(k, 2 * i)):
                solution_ref[step, 2 * i + u] = one

    rows_to_cells(BACK, 5, 3)

    for at in range(PIECES // 2):
        arrived(beside_received.at[pl.ds(0, 7 * 8)], beside_send.at[at], beside_recv.at[at])
    both = jnp.concatenate([beside_received[pl.ds(side, N, stride=2), :] for side in range(2)], axis=1)
    both = along_columns(left_ref[...], both)
    both = along_rows(jnp.concatenate([both[:, :N], both[:, N:]], axis=0), right_ref)
    beside_cells[pl.ds(0, 2)] = both.reshape(2, N, N)

    @pl.loop(0, 16)
    def _(x):
        beside_cells[x + 2] = solution_ref[0, x] - solution_ref[2, x]

    beside_cells[18] = beside_cells[1]
    beside_cells[1] = beside_cells[0]

    @pl.loop(0, 8, unroll=True)
    def _(i):
        for u, one in enumerate(to_cells(BACK, 2 * i)):
            x = 2 * i + u
            bent = beside_cells[x + 1] + beside_cells[x + 3] - 2.0 * beside_cells[x + 2] + one
            total = solution_ref[0, x] + solution_ref[2, x] + HALF_STEP * bent
            solution_ref[1, x] = 0.5 * total + HALF_STEP * gap_cells[x + 1]

    back(2, late)
    rows_to_cells(2, 5, 3)

    @pl.loop(0, 8, unroll=True)
    def _(i):
        for u, one in enumerate(to_cells(2, 2 * i)):
            solution_ref[3, 2 * i + u] = one

    for at in range(PIECES // 2):
        left_here(beside_received.at[pl.ds(0, 7 * 8)], beside_send.at[at], beside_recv.at[at])
    for k in range(BACK):
        at = PIECES * (k + 1) - 1
        left_here(back_received.at[0, pl.ds(0, 7 * 32)], back_send.at[at], back_recv.at[at])

def per_device(forcing, coarse_guess, initial):
    modal = (HALVES, PAIRS, N, 2 * N)
    quarters = PIECES // 2
    dma = pltpu.SemaphoreType.DMA
    vmem = pl.BlockSpec(memory_space=pltpu.VMEM)
    anywhere = pl.BlockSpec(memory_space=pltpu.HBM)
    given = tuple(jnp.asarray(one) for one in tables())
    out, gap = pl.pallas_call(
        kernel,
        out_shape=(
            jax.ShapeDtypeStruct((STEPS, 16, N, N), F32),
            jax.ShapeDtypeStruct((16 * N, N), F32),
        ),
        in_specs=[anywhere] * (3 + len(given)),
        out_specs=(vmem, vmem),
        scratch_shapes=[
            pltpu.VMEM((STEPS + 1, 16, N, N), F32),
            pltpu.VMEM((16, N, N), F32),
            pltpu.VMEM((18, N, N), F32),
            pltpu.VMEM((2 * FIELDS, SPACE, N, N), F32),
            pltpu.VMEM((2 * FIELDS, SPACE * N, N), F32),
            pltpu.VMEM((1024, N), F32),
            pltpu.VMEM((SPACE, N, N), F32),
            pltpu.VMEM((SPACE, N, N), F32),
            pltpu.VMEM((PIECES, ROWS, N), F32),
            pltpu.VMEM(modal, F32),
            pltpu.VMEM(modal, F32),
            pltpu.VMEM(modal, F32),
            pltpu.VMEM(modal, F32),
            pltpu.VMEM(modal, F32),
            pltpu.VMEM((3,) + modal, F32),
            pltpu.VMEM(modal, F32),
            pltpu.VMEM(modal, F32),
            pltpu.VMEM((PIECES, TM, ROWS, N), F32),
            pltpu.VMEM((PIECES, TM, ROWS, N), F32),
            pltpu.VMEM(modal, F32),
            pltpu.VMEM((BACK * PIECES, SPACE, 32, N), F32),
            pltpu.VMEM((BACK + 1, 16 * N, N), F32),
            pltpu.VMEM((quarters, 64, N), F32),
            pltpu.VMEM((2 * N, N), F32),
            pltpu.VMEM((19, N, N), F32),
            dma((STEPS + 2,)),
            dma((2 * FIELDS,)),
            dma((2 * FIELDS,)),
            dma((2,)),
            dma((2,)),
            dma,
            dma,
            dma((HALVES,)),
            dma((HALVES,)),
            dma((PIECES,)),
            dma((PIECES,)),
            dma((PIECES,)),
            dma((PIECES,)),
            dma((PIECES,)),
            dma((PIECES,)),
            dma((BACK * PIECES,)),
            dma((BACK * PIECES,)),
            dma((quarters,)),
            dma((quarters,)),
            pltpu.SemaphoreType.REGULAR((4,)),
            dma((len(given),)),
        ] + [pltpu.VMEM(one.shape, one.dtype) for one in given] + [
        ],
        compiler_params=pltpu.CompilerParams(
            collective_id=0, has_side_effects=True, vmem_limit_bytes=46 * 1024 * 1024
        ),
    )(*(pltpu.with_memory_space_constraint(one, pltpu.HBM) for one in (forcing, coarse_guess, initial) + given))
    return out, gap.reshape(1, N, 16, N)


def solution(mesh):
    in_specs = (P("tm", "space", None, None), P("tm", "space", None, None), P("space", None, None))
    out_specs = (P("tm", "space", None, None), P("tm", None, "space", None))
    return jax.shard_map(per_device, mesh=mesh, in_specs=in_specs, out_specs=out_specs, check_vma=False)
```
